128 devices in a mesh: row: 16 (over y, x_lo, core), col: 8 (over x_hi, z).
Axes of the slice: x: 4 (x_hi: 2, x_lo: 2; x = x_hi * 2 + x_lo), y: 4, z: 4, core: 2. Of those that a mesh axis runs over, the one named last changes fastest.
Arguments:
- coeffs: bfloat16 [65536, 2048], P('row', 'col'), may hold values from -0.8984375 to 0.8984375
- occupations: float32 [2048], replicated, may hold values from 0.05 to 2
- block_order: int32 [128], replicated, may hold values from 0 to 127, as said below
- neighbours: int32 [128, 15], P(('row', 'col')), may hold values from 0 to 127, as said below
- counts: int32 [128], P(('row', 'col')), may hold values from 4 to 15, as said below
Outputs:
- density: bfloat16 [128, 15, 512, 512], P(('row', 'col'))
The draws below stay inside these ranges and needn't reach their ends.
Inputs may be any that keep to these rules, and one draw needn't show every extreme that they name: Within each aligned group of 8 entries, block_order is a permutation of that group's own indices. For atom row block a, the first counts[a] entries of neighbours[a] are distinct blocks b with |b - a| < 8; the remaining entries equal a. `counts`: some block has 15 live slots in every draw.
All inputs are finite; a program needn't handle non-finite values.
Results may differ from the reference program's by a relative error of at most 0.0044.
Values may be sent and summed in bfloat16 or wider, within the bound.
No kernel may reach another device: no remote copies, remote signals or barrier semaphores. Data moves between devices by JAX's collectives and lax.ppermute only.
A program may use at most 128 MiB of HBM per device.

```python
import jax
import jax.numpy as jnp
from jax import lax

BS = 512
STATES = 2048
W = 8
NNB = 15
NBLK = 128
NB = 65536
N_COL = 8


def pattern_draw(key):
    base = jax.random.fold_in(key, 71)
    offsets = jnp.arange(NNB, dtype=jnp.int32) - (W - 1)
    row_keys = jax.random.split(jax.random.fold_in(base, 1), NBLK)
    shuffled = jax.vmap(lambda k: jax.random.permutation(k, offsets))(row_keys)
    blocks = jnp.arange(NBLK, dtype=jnp.int32)
    targets = blocks[:, None] + shuffled
    valid = (targets >= 0) & (targets < NBLK) & (shuffled != 0)
    ranks = jnp.argsort(jnp.where(valid, 0, 1).astype(jnp.int32), axis=1, stable=True)
    targets = jnp.take_along_axis(targets, ranks, axis=1)
    available = jnp.sum(valid.astype(jnp.int32), axis=1) + 1
    wanted = jax.random.randint(jax.random.fold_in(base, 2), (NBLK,), 4, NNB + 1).astype(jnp.int32)
    heavy = jax.random.randint(jax.random.fold_in(base, 3), (), W, NBLK - W + 1).astype(jnp.int32)
    wanted = jnp.where(blocks == heavy, NNB, wanted)
    live = jnp.minimum(wanted, available)
    own_first = jnp.concatenate([blocks[:, None], targets[:, :NNB - 1]], axis=1)
    slots = jnp.arange(NNB, dtype=jnp.int32)[None, :]
    lists = jnp.where(slots < live[:, None], own_first, blocks[:, None])
    return (lists.astype(jnp.int32), live.astype(jnp.int32))


def draw_neighbours(key, part):
    return pattern_draw(key)[0]


def draw_counts(key, part):
    return pattern_draw(key)[1]


def draw_block_order(key, part):
    group_keys = jax.random.split(jax.random.fold_in(key, 5), NBLK // N_COL)
    perms = jax.vmap(lambda k: jax.random.permutation(k, N_COL))(group_keys).astype(jnp.int32)
    bases = (jnp.arange(NBLK // N_COL, dtype=jnp.int32) * N_COL)[:, None]
    return (perms + bases).reshape(NBLK).astype(jnp.int32)


def level_of(key, shape, shards, smallest, high):
    def one(position, shards_of):
        heights = jax.random.uniform(jax.random.fold_in(jax.random.fold_in(key, 6), position), (shards_of,), jnp.float32, smallest / len(shards), high / len(shards))
        return jnp.repeat(jnp.exp(heights), shape[position] // shards_of).reshape((-1,) + (1,) * (len(shape) - position - 1))

    factor_of = one(*shards[0])
    for cut in shards[1:]:
        factor_of = factor_of * one(*cut)
    return factor_of


def noise(key, extent, scale, bound, cuts=(), kind=jnp.bfloat16):
    values = scale * jax.random.normal(key, extent, jnp.float32)
    if cuts:
        values = values * level_of(key, extent, cuts, -0.22, 0.18)
    return jnp.clip(values, -bound, bound).astype(kind)


def setup_inputs(seed: int = 0) -> dict:
    keys = jax.random.split(jax.random.key(seed), 6)
    coeffs = noise(keys[0], (NB, STATES), 0.15, 0.8984375, ((0, 16), (1, 8)))
    occupations = jnp.clip(jax.random.uniform(keys[1], (STATES,), jnp.float32, 0.05, 2.0), 0.05, 2.0)
    block_order = draw_block_order(jax.random.fold_in(keys[5], 71), 0)
    neighbours = draw_neighbours(jax.random.fold_in(keys[5], 71), 0)
    counts = draw_counts(jax.random.fold_in(keys[5], 71), 0)
    return dict(coeffs=coeffs, occupations=occupations, block_order=block_order, neighbours=neighbours, counts=counts)


def reference(coeffs, occupations, block_order, neighbours, counts):
    atoms = coeffs.reshape(NBLK, BS, STATES)[block_order.astype(jnp.int32)]
    weighted = (atoms.astype(jnp.float32) * occupations[None, None, :]).astype(jnp.bfloat16)
    slots = jnp.arange(NNB, dtype=jnp.int32)

    def one_block(items):
        weight_rows, partner, live_count = items
        chosen = atoms[partner.astype(jnp.int32)].astype(jnp.float32)
        products = jnp.einsum("ik,jnk->jin", weight_rows.astype(jnp.float32), chosen)
        live = (slots < live_count)[:, None, None]
        return jnp.where(live, products, jnp.zeros_like(products)).astype(jnp.bfloat16)

    return lax.map(one_block, (weighted, neighbours, counts))
```

```python
import functools

import jax
import jax.numpy as jnp
from jax import lax
from jax.experimental import pallas as pl
from jax.experimental.pallas import tpu as pltpu
from jax.sharding import PartitionSpec as P

W = 8
NNB = 15
BS = 512
COLS = 8
KS = 256
AXES = ("row", "col")
TILE = 256


def devices():
    for k in range(8):
        for core in range(2):
            for xh in range(2):
                for z in range(4):
                    yield k, core, xh, z


def index(k, core, xh, z):
    return ((k * 2 + core) * 2 + xh) * 4 + z


def group_route(dx, dz):
    return [(index(k, c, x ^ dx, (z + dz) % 4), index(k, c, x, z)) for k, c, x, z in devices()]


def swap_route():
    return [(index(k, c, x, z), index(k, 1 - c, x, z)) for k, c, x, z in devices()]


def partner_of(k, core):
    return (k + 1, 0) if core else (k - 1, 1)


def edge_route():
    pairs = []
    for k, c, x, z in devices():
        to, tc = partner_of(k, c)
        if 0 <= to < 8:
            pairs.append((index(k, c, x, z), index(to, tc, x, z)))
    return pairs


def result_route(dx, dz):
    pairs = []
    for k, c, x, z in devices():
        j = x * 4 + z
        v = (x ^ dx) * 4 + (z + dz) % 4
        if (v > j) != bool(c):
            to, tc = k, 1 - c
        else:
            to, tc = partner_of(k, c)
        if 0 <= to < 8:
            pairs.append((index(k, c, x, z), index(to, tc, x, z)))
    return pairs


def send(value, route):
    return lax.ppermute(value, AXES, route)


def place(dx, dz):
    core = lax.rem(lax.axis_index("row"), 2)
    j = lax.axis_index("col")
    x, z = lax.div(j, 4), lax.rem(j, 4)
    vx = 1 - x if dx else x
    return core, j, vx * 4 + lax.rem(z + dz, 4)


def slot_for(neighbours, counts, offset):
    own = lax.axis_index("row") * COLS + lax.axis_index("col")
    slot = jnp.int32(NNB)
    for s in range(NNB):
        hit = (neighbours[0, s] == own + offset) & (s < counts[0])
        slot = jnp.where(hit, s, slot)
    return slot


def load(parts, target, sem):
    copies, c = [], 0
    for part in parts:
        for i in range(part.shape[0]):
            copies.append(pltpu.make_async_copy(part.at[i], target.at[:, pl.ds(c * KS, KS)], sem))
            c += 1
    return copies


def multiply(left, right, result):
    def step(n, _):
        rows = pl.ds(pl.multiple_of(n * TILE, TILE), TILE)
        result[:, rows] = lax.dot_general(
            left[...], right[rows, :], (((1,), (1,)), ((), ())), preferred_element_type=jnp.float32
        ).astype(jnp.bfloat16)
        return 0

    lax.fori_loop(0, BS // TILE, step, 0)


def own_kernel(dx, dz, first, n_parts, neighbours, counts, weights, *rest):
    parts, rest = rest[:n_parts], rest[n_parts:]
    if not first:
        rest = rest[1:]
    out, left, right, result, sem, out_sem = rest
    _, j, v = place(dx, dz)
    slot = slot_for(neighbours, counts, v - j)
    if first:
        result[...] = jnp.zeros_like(result)
        for s in range(NNB):
            @pl.when(s >= counts[0])
            def _():
                pltpu.make_async_copy(result, out.at[s], out_sem).start()
        for s in range(NNB):
            @pl.when(s >= counts[0])
            def _():
                pltpu.make_async_copy(result, out.at[s], out_sem).wait()

    @pl.when(slot < NNB)
    def _():
        copies = load([weights], left, sem) + load(parts, right, sem)
        for copy in copies:
            copy.start()
        for copy in copies:
            copy.wait()
        multiply(left, right, result)
        store = pltpu.make_async_copy(result, out.at[slot], out_sem)
        store.start()
        store.wait()


def query_kernel(dx, dz, n_parts, near, far, *rest):
    parts, (out, left, right, sem) = rest[:n_parts], rest[n_parts:]
    core, j, v = place(dx, dz)
    use_near = jnp.where(core == 0, v > j, v < j)

    @pl.when(use_near)
    def _():
        for copy in load([near], left, sem):
            copy.start()

    @pl.when(jnp.logical_not(use_near))
    def _():
        for copy in load([far], left, sem):
            copy.start()

    copies = load(parts, right, sem)
    for copy in copies:
        copy.start()
    for copy in copies + load([near], left, sem):
        copy.wait()
    multiply(left, right, out)


def gather_kernel(steps, neighbours, counts, *rest):
    n = len(steps)
    results, (_, out, held, sem, out_sem) = rest[:n], rest[n:]
    for i in range(n):
        pltpu.make_async_copy(results[i], held.at[i], sem.at[i]).start()
    for i, (dx, dz) in enumerate(steps):
        _, j, v = place(dx, dz)
        slot = slot_for(neighbours, counts, jnp.where(v < j, 8 + v - j, v - j - 8))
        pltpu.make_async_copy(results[i], held.at[i], sem.at[i]).wait()

        @pl.when(slot < NNB)
        def _():
            store = pltpu.make_async_copy(held.at[i], out.at[slot], out_sem)
            store.start()
            store.wait()


ANY = pl.BlockSpec(memory_space=pl.ANY)
SMEM = pl.BlockSpec(memory_space=pltpu.SMEM)
VMEM = pl.BlockSpec(memory_space=pltpu.VMEM)
OUT = jax.ShapeDtypeStruct((NNB, BS, BS), jnp.bfloat16)
RESULT = jax.ShapeDtypeStruct((BS, BS), jnp.bfloat16)
BLOCK = pltpu.VMEM((BS, COLS * KS), jnp.bfloat16)
COST = pl.CostEstimate(flops=2 * BS * BS * COLS * KS, bytes_accessed=9 * BS * BS, transcendentals=0)


def own_product(step, neighbours, counts, weights, parts, out):
    first = out is None
    extra = [] if first else [out]
    n = len(parts)
    return pl.pallas_call(
        functools.partial(own_kernel, *step, first, n),
        out_shape=OUT,
        in_specs=[SMEM, SMEM] + [ANY] * (1 + n + len(extra)),
        out_specs=ANY,
        scratch_shapes=[
            BLOCK, BLOCK, pltpu.VMEM((BS, BS), jnp.bfloat16),
            pltpu.SemaphoreType.DMA, pltpu.SemaphoreType.DMA,
        ],
        input_output_aliases={} if first else {3 + n: 0},
        cost_estimate=COST,
        compiler_params=pltpu.CompilerParams(vmem_limit_bytes=24 << 20),
        name="own_product",
    )(neighbours, counts, weights, *parts, *extra)


def query_product(step, near, far, parts):
    n = len(parts)
    return pl.pallas_call(
        functools.partial(query_kernel, *step, n),
        out_shape=RESULT,
        in_specs=[ANY] * (2 + n),
        out_specs=VMEM,
        scratch_shapes=[BLOCK, BLOCK, pltpu.SemaphoreType.DMA],
        cost_estimate=COST,
        compiler_params=pltpu.CompilerParams(vmem_limit_bytes=24 << 20),
        name="query_product",
    )(near, far, *parts)


def gather(steps, neighbours, counts, results, out):
    n = len(steps)
    return pl.pallas_call(
        functools.partial(gather_kernel, steps),
        out_shape=OUT,
        in_specs=[SMEM, SMEM] + [ANY] * (n + 1),
        out_specs=ANY,
        scratch_shapes=[
            pltpu.VMEM((n, BS, BS), jnp.bfloat16),
            pltpu.SemaphoreType.DMA((n,)), pltpu.SemaphoreType.DMA,
        ],
        input_output_aliases={2 + n: 0},
        compiler_params=pltpu.CompilerParams(vmem_limit_bytes=16 << 20),
        name="place_results",
    )(neighbours, counts, *results, out)


def shards(coeffs, occupations, block_order, neighbours, counts):
    group_base = lax.axis_index("row") * COLS
    local = coeffs.reshape(COLS, BS, KS)
    picks = lax.dynamic_slice_in_dim(block_order, group_base, COLS) - group_base
    own = lax.all_to_all(local[picks], "col", split_axis=0, concat_axis=0, tiled=True)
    scale = occupations.reshape(COLS, 1, KS)
    weights = (own.astype(jnp.float32) * scale).astype(jnp.bfloat16)

    half = COLS // 2
    across = send(own, group_route(1, 0))
    back = send(own, group_route(0, 3))
    ahead = send(own, group_route(0, 1))
    near = send(weights, swap_route())
    weights_late, across = lax.optimization_barrier((weights, across))
    far = send(weights_late, edge_route())
    twice_back = send(back[:half], group_route(0, 3))
    twice_ahead = send(ahead[half:], group_route(0, 1))
    across_back = send(across, group_route(0, 3))
    across_ahead = send(across, group_route(0, 1))
    across_twice_back = send(across_back[:half], group_route(0, 3))
    across_twice_ahead = send(across_ahead[half:], group_route(0, 1))

    arrivals = [
        ((0, 3), [back]),
        ((0, 1), [ahead]),
        ((1, 0), [across]),
        ((0, 2), [twice_back, twice_ahead]),
        ((1, 3), [across_back]),
        ((1, 1), [across_ahead]),
        ((1, 2), [across_twice_back, across_twice_ahead]),
    ]
    out = own_product((0, 0), neighbours, counts, weights, [own], None)
    results = []
    for step, parts in arrivals:
        out = own_product(step, neighbours, counts, weights, parts, out)
        results.append(send(query_product(step, near, far, parts), result_route(*step)))
    out = gather([step for step, _ in arrivals], neighbours, counts, results, out)
    return out[None]


def solution(mesh):
    return jax.shard_map(
        shards,
        mesh=mesh,
        in_specs=(P("row", "col"), P(), P(), P(("row", "col"), None), P(("row", "col"))),
        out_specs=P(("row", "col"), None, None, None),
        check_vma=False,
    )
```

```python
import functools

import jax
import jax.numpy as jnp
from jax import lax
from jax.experimental import pallas as pl
from jax.experimental.pallas import tpu as pltpu
from jax.sharding import PartitionSpec as P


NNB = 15
BS = 512
COLS = 8
KS = 256
STATES = COLS * KS
AXES = ("row", "col")
TILE = 256


def devices():
    for k in range(8):
        for core in range(2):
            for xh in range(2):
                for z in range(4):
                    yield k, core, xh, z


def index(k, core, xh, z):
    return ((k * 2 + core) * 2 + xh) * 4 + z


def up_of(core):
    return -1 if core else 1


def move_route(dx, up):
    return [
        (index(k, c, x ^ dx, (z - up * up_of(c)) % 4), index(k, c, x, z)) for k, c, x, z in devices()
    ]


def swap_route():
    return [(index(k, c, x, z), index(k, 1 - c, x, z)) for k, c, x, z in devices()]


def partner_of(k, core):
    return (k + 1, 0) if core else (k - 1, 1)


def edge_route():
    pairs = []
    for k, c, x, z in devices():
        to, tc = partner_of(k, c)
        if 0 <= to < 8:
            pairs.append((index(k, c, x, z), index(to, tc, x, z)))
    return pairs


def result_route(t, r):
    pairs = []
    for k, c, x, z in devices():
        j = x * 4 + z
        v = (x ^ t) * 4 + (z + r * up_of(c)) % 4
        if (v > j) != bool(c):
            to, tc = k, 1 - c
        else:
            to, tc = partner_of(k, c)
        if 0 <= to < 8:
            pairs.append((index(k, c, x, z), index(to, tc, x, z)))
    return pairs


def send(value, route):
    return lax.ppermute(value, AXES, route)


def where_am_i():
    core = lax.rem(lax.axis_index("row"), 2)
    j = lax.axis_index("col")
    return core, j, lax.div(j, 4), lax.rem(j, 4)


def around(z, core, ups):
    return lax.rem(z + 4 + jnp.where(core == 0, ups, -ups), 4)


def place(t, r):
    core, j, x, z = where_am_i()
    return core, j, (1 - x if t else x) * 4 + around(z, core, r)


def slot_for(neighbours, counts, offset):
    own = lax.axis_index("row") * COLS + lax.axis_index("col")
    slot = jnp.int32(NNB)
    for s in range(NNB):
        hit = (neighbours[0, s] == own + offset) & (s < counts[0])
        slot = jnp.where(hit, s, slot)
    return slot


def result_slot(neighbours, counts, t, r, opposite):
    _, j, v = place(t, -r if opposite else r)
    return slot_for(neighbours, counts, jnp.where(v < j, 8 + v - j, v - j - 8))


def columns(c):
    return pl.ds(c * KS, KS)


def load(parts, target, sem):
    return [
        pltpu.make_async_copy(ref.at[i], target.at[:, columns(c)], sem)
        for c, (ref, i) in enumerate(parts)
    ]


MIRROR = (0, 3, 2, 1, 4, 7, 6, 5)


def load_mirrored(whole, target, sem):
    return [
        pltpu.make_async_copy(whole.at[:, columns(m)], target.at[:, columns(c)], sem)
        for c, m in enumerate(MIRROR)
    ]


def multiply(left, right, result):
    def step(n, _):
        rows = pl.ds(pl.multiple_of(n * TILE, TILE), TILE)
        result[:, rows] = lax.dot_general(
            left[...], right[rows, :], (((1,), (1,)), ((), ())), preferred_element_type=jnp.float32
        ).astype(jnp.bfloat16)
        return 0

    lax.fori_loop(0, BS // TILE, step, 0)


def pick_kernel(block_order, coeffs, a0, y0, a1, y1, sem):
    core, _, x, z = where_am_i()
    base = lax.axis_index("row") * COLS
    copies = []
    for t, (a, y) in enumerate(((a0, y0), (a1, y1))):
        for ref, rs in ((a, (2, 1)), (y, (3, 0))):
            for i, r in enumerate(rs):
                v = (1 - x if t else x) * 4 + around(z, core, r)
                copies.append(pltpu.make_async_copy(coeffs.at[block_order[base + v] - base], ref.at[i], sem))
    for copy in copies:
        copy.start()
    for copy in copies:
        copy.wait()


def n_arrays(where):
    return max(i for parts in where for i, _ in parts) + 1


def weigh_kernel(where, occupations, *rest):
    refs, (out, block, sem) = rest[:-3], rest[-3:]
    copies = load([(refs[n], i) for n, i in where[0]], block, sem)
    for copy in copies:
        copy.start()
    for copy in copies:
        copy.wait()
    core, _, x, z = where_am_i()
    for c in range(COLS):
        ups = (0, -1, -2, 1)[c % 4]
        source = (1 - x if c // 4 else x) * 4 + around(z, core, ups)
        scale = occupations[pl.ds(source, 1), :]
        out[:, columns(c)] = (block[:, columns(c)].astype(jnp.float32) * scale).astype(jnp.bfloat16)


def own_kernel(blocks, first, where, neighbours, counts, weights, *rest):
    n = len(blocks)
    refs, rest = rest[: n_arrays(where)], rest[n_arrays(where) :]
    if not first:
        rest = rest[1:]
    out, left, right, result, left_sem, sem, out_sem = rest
    slots = []
    for b, (t, r) in enumerate(blocks):
        _, j, v = place(t, r)
        slots.append(slot_for(neighbours, counts, v - j))
    pltpu.make_async_copy(weights, left, left_sem).start()
    for b in range(n):
        @pl.when(slots[b] < NNB)
        def _():
            for copy in load([(refs[i], p) for i, p in where[b]], right.at[b], sem.at[b]):
                copy.start()

    if first:
        result[0] = jnp.zeros((BS, BS), jnp.bfloat16)
        for s in range(NNB):
            @pl.when(s >= counts[0])
            def _():
                pltpu.make_async_copy(result.at[0], out.at[s], out_sem.at[0]).start()
        for s in range(NNB):
            @pl.when(s >= counts[0])
            def _():
                pltpu.make_async_copy(result.at[0], out.at[s], out_sem.at[0]).wait()
    pltpu.make_async_copy(weights, left, left_sem).wait()
    for b in range(n):
        @pl.when(slots[b] < NNB)
        def _():
            for copy in load([(refs[i], p) for i, p in where[b]], right.at[b], sem.at[b]):
                copy.wait()
            multiply(left, right.at[b], result.at[b])
            pltpu.make_async_copy(result.at[b], out.at[slots[b]], out_sem.at[b]).start()
    for b in range(n):
        @pl.when(slots[b] < NNB)
        def _():
            pltpu.make_async_copy(result.at[b], out.at[slots[b]], out_sem.at[b]).wait()


def ask_kernel(blocks, where, near, far, *rest):
    n = len(blocks)
    refs, rest = rest[: n_arrays(where)], rest[n_arrays(where) :]
    outs, (left, right, left_sem, sem) = rest[:-4], rest[-4:]
    core, j, v = place(*blocks[0])
    alike = all(t == 1 for t, _ in blocks)
    if alike:
        use_near = jnp.where(core == 0, v > j, v < j)

        @pl.when(use_near)
        def _():
            for copy in load_mirrored(near, left.at[0], left_sem):
                copy.start()

        @pl.when(jnp.logical_not(use_near))
        def _():
            for copy in load_mirrored(far, left.at[0], left_sem):
                copy.start()
    else:
        for copy in load_mirrored(near, left.at[0], left_sem) + load_mirrored(far, left.at[1], left_sem):
            copy.start()
    for b in range(n):
        for copy in load([(refs[i], p) for i, p in where[b]], right.at[b], sem.at[b]):
            copy.start()
    for copy in load_mirrored(near, left.at[0], left_sem):
        copy.wait()
    if not alike:
        for copy in load_mirrored(far, left.at[1], left_sem):
            copy.wait()
    for b in range(n):
        for copy in load([(refs[i], p) for i, p in where[b]], right.at[b], sem.at[b]):
            copy.wait()
        _, _, v = place(*blocks[b])
        chosen = 0 if alike else jnp.where(jnp.where(core == 0, v > j, v < j), 0, 1)
        multiply(left.at[chosen], right.at[b], outs[0].at[b] if alike else outs[b])


def gather_kernel(steps, where, neighbours, counts, *rest):
    n = len(steps)
    refs, (_, out, held, sem, out_sem) = rest[:-5], rest[-5:]
    sources = [refs[i] if p is None else refs[i].at[p] for i, p in where]
    for i in range(n):
        pltpu.make_async_copy(sources[i], held.at[i], sem.at[i]).start()
    slots = []
    for i, (t, r) in enumerate(steps):
        slots.append(result_slot(neighbours, counts, t, r, True))
        pltpu.make_async_copy(sources[i], held.at[i], sem.at[i]).wait()

        @pl.when(slots[i] < NNB)
        def _():
            pltpu.make_async_copy(held.at[i], out.at[slots[i]], out_sem.at[i]).start()

    for i in range(n):
        @pl.when(slots[i] < NNB)
        def _():
            pltpu.make_async_copy(held.at[i], out.at[slots[i]], out_sem.at[i]).wait()


ANY = pl.BlockSpec(memory_space=pl.ANY)
SMEM = pl.BlockSpec(memory_space=pltpu.SMEM)
VMEM = pl.BlockSpec(memory_space=pltpu.VMEM)
OUT = jax.ShapeDtypeStruct((NNB, BS, BS), jnp.bfloat16)
RESULT = jax.ShapeDtypeStruct((BS, BS), jnp.bfloat16)
PAIR = jax.ShapeDtypeStruct((2, BS, KS), jnp.bfloat16)
WHOLE = jax.ShapeDtypeStruct((BS, STATES), jnp.bfloat16)
BLOCK = pltpu.VMEM((BS, STATES), jnp.bfloat16)


def cost(n):
    return pl.CostEstimate(flops=n * 2 * BS * BS * STATES, bytes_accessed=n * 9 * BS * BS, transcendentals=0)


def limit(mib):
    return pltpu.CompilerParams(vmem_limit_bytes=mib << 20)


def pick(block_order, coeffs):
    return pl.pallas_call(
        pick_kernel,
        out_shape=[PAIR] * 4,
        in_specs=[SMEM, ANY],
        out_specs=[VMEM] * 4,
        scratch_shapes=[pltpu.SemaphoreType.DMA],
        compiler_params=limit(8),
        name="pick",
    )(block_order, coeffs)


def distinct(blocks):
    arrays, where = [], []
    for parts in blocks:
        row = []
        for array, position in parts:
            n = next((i for i, other in enumerate(arrays) if other is array), len(arrays))
            if n == len(arrays):
                arrays.append(array)
            row.append((n, position))
        where.append(tuple(row))
    return arrays, tuple(where)


def weigh(occupations, parts):
    arrays, where = distinct([parts])
    return pl.pallas_call(
        functools.partial(weigh_kernel, where),
        out_shape=WHOLE,
        in_specs=[VMEM] + [ANY] * len(arrays),
        out_specs=VMEM,
        scratch_shapes=[BLOCK, pltpu.SemaphoreType.DMA],
        compiler_params=limit(12),
        name="weigh",
    )(occupations, *arrays)


def own_products(blocks, neighbours, counts, weights, parts, out):
    first = out is None
    extra = [] if first else [out]
    arrays, where = distinct(parts)
    m, n = len(arrays), len(blocks)
    return pl.pallas_call(
        functools.partial(own_kernel, blocks, first, where),
        out_shape=OUT,
        in_specs=[SMEM, SMEM] + [ANY] * (1 + m + len(extra)),
        out_specs=ANY,
        scratch_shapes=[
            BLOCK, pltpu.VMEM((n, BS, STATES), jnp.bfloat16), pltpu.VMEM((n, BS, BS), jnp.bfloat16),
            pltpu.SemaphoreType.DMA, pltpu.SemaphoreType.DMA((n,)), pltpu.SemaphoreType.DMA((n,)),
        ],
        input_output_aliases={} if first else {3 + m: 0},
        cost_estimate=cost(n),
        compiler_params=limit(20),
        name="own_products",
    )(neighbours, counts, weights, *arrays, *extra)


def ask_products(blocks, near, far, parts):
    arrays, where = distinct(parts)
    n = len(blocks)
    alike = all(t == 1 for t, _ in blocks)
    return pl.pallas_call(
        functools.partial(ask_kernel, blocks, where),
        out_shape=jax.ShapeDtypeStruct((n, BS, BS), jnp.bfloat16) if alike else [RESULT] * n,
        in_specs=[ANY] * (2 + len(arrays)),
        out_specs=VMEM if alike else [VMEM] * n,
        scratch_shapes=[
            pltpu.VMEM((1 if alike else 2, BS, STATES), jnp.bfloat16),
            pltpu.VMEM((n, BS, STATES), jnp.bfloat16),
            pltpu.SemaphoreType.DMA, pltpu.SemaphoreType.DMA((n,)),
        ],
        cost_estimate=cost(n),
        compiler_params=limit(20),
        name="ask_products",
    )(near, far, *arrays)


def gather(steps, neighbours, counts, results, out):
    arrays, where = distinct([results])
    n = len(steps)
    return pl.pallas_call(
        functools.partial(gather_kernel, steps, where[0]),
        out_shape=OUT,
        in_specs=[SMEM, SMEM] + [ANY] * (len(arrays) + 1),
        out_specs=ANY,
        scratch_shapes=[
            pltpu.VMEM((n, BS, BS), jnp.bfloat16),
            pltpu.SemaphoreType.DMA((n,)), pltpu.SemaphoreType.DMA((n,)),
        ],
        input_output_aliases={2 + len(arrays): 0},
        compiler_params=limit(8),
        name="place_results",
    )(neighbours, counts, *arrays, out)


def shards(coeffs, occupations, block_order, neighbours, counts):
    local = pick(block_order, coeffs.reshape(COLS, BS, KS))
    held = {("O", 0, "A"): local[0], ("O", 0, "Y"): local[1], ("O", 1, "A"): local[2], ("O", 1, "Y"): local[3]}
    up, down, far_up = {}, {}, {}
    for t in range(2):
        for part in "AY":
            held["P", t, part] = send(held["O", 1 - t, part], move_route(1, 0))
    for key in [(x, t, part) for t in range(2) for x in "OP" for part in "AY"]:
        up[key] = send(held[key], move_route(0, 1))
        down[key] = send(held[key], move_route(0, -1))
        if key[1:] == (1, "Y"):
            other = far_up["P" if key[0] == "O" else "O", 0, "Y"]
            far_up[key] = send(other, move_route(1, 0))
        else:
            far_up[key] = send(up[key], move_route(0, 1))

    own_at = {2: ("A", 0), 1: ("A", 1), 3: ("Y", 0), 0: ("Y", 1)}

    def parts_of(t, r):
        parts = []
        for x in "OP":
            for table, shift in ((held, 0), (up, 1), (far_up, 2), (down, -1)):
                part, position = own_at[(r + shift) % 4]
                parts.append((table[x, t, part], position))
        return parts

    weights = weigh(occupations.reshape(COLS, KS), parts_of(0, 0))
    near = send(weights, swap_route())
    far = send(weights, edge_route())
    out = own_products(((0, 0),), neighbours, counts, weights, [parts_of(0, 0)], None)

    half = ((0, 3), (0, 1), (0, 2))
    parts = [parts_of(*b) for b in half]
    out = own_products(half, neighbours, counts, weights, parts, out)
    answers = ask_products(half, near, far, parts)
    back = [(send(a, result_route(*b)), None) for a, b in zip(answers, half)]
    early, late = ((1, 0), (1, 1)), ((1, 3), (1, 2))
    for pair in (early, late):
        parts = [parts_of(*b) for b in pair]
        answer = ask_products(pair, near, far, parts)
        answer = send(answer, result_route(*pair[0]))
        back += [(answer, 0), (answer, 1)]
        out = own_products(pair, neighbours, counts, weights, parts, out)
    out = gather(half + early, neighbours, counts, back[:5], out)
    out = gather(late, neighbours, counts, back[5:], out)
    return out[None]


def solution(mesh):
    return jax.shard_map(
        shards,
        mesh=mesh,
        in_specs=(P("row", "col"), P(), P(), P(("row", "col"), None), P(("row", "col"))),
        out_specs=P(("row", "col"), None, None, None),
        check_vma=False,
    )
```

```python
import functools

import jax
import jax.numpy as jnp
from jax import lax
from jax.experimental import pallas as pl
from jax.experimental.pallas import tpu as pltpu
from jax.sharding import PartitionSpec as P


NNB = 15
BS = 512
COLS = 8
KS = 256
STATES = COLS * KS
AXES = ("row", "col")
TILE = 256


def devices():
    for k in range(8):
        for core in range(2):
            for xh in range(2):
                for z in range(4):
                    yield k, core, xh, z


def index(k, core, xh, z):
    return ((k * 2 + core) * 2 + xh) * 4 + z


def up_of(core):
    return -1 if core else 1


def move_route(dx, up):
    return [
        (index(k, c, x ^ dx, (z - up * up_of(c)) % 4), index(k, c, x, z)) for k, c, x, z in devices()
    ]


def swap_route():
    return [(index(k, c, x, z), index(k, 1 - c, x, z)) for k, c, x, z in devices()]


def partner_of(k, core):
    return (k + 1, 0) if core else (k - 1, 1)


def in_plane(k, core):
    return (k % 2 == 0) != (core == 0)


def edge_route():
    pairs = []
    for k, c, x, z in devices():
        to, tc = partner_of(k, c)
        if 0 <= to < 8 and in_plane(k, c):
            pairs.append((index(k, c, x, z), index(to, tc, x, z)))
    return pairs


def plane_routes():
    first, second = [], []
    for k, c, x, z in devices():
        to, tc = partner_of(k, c)
        if 0 <= to < 8 and not in_plane(k, c):
            middle = index(2 * to - k, c, x, z)
            first.append((index(k, c, x, z), middle))
            second.append((middle, index(to, tc, x, z)))
    return first, second


def asks_near(core, xh):
    return (core == 0) == (xh == 0)


def across_route():
    pairs = []
    for k, c, x, z in devices():
        to, tc = partner_of(k, c)
        if 0 <= to < 8 and asks_near(c, x):
            pairs.append((index(k, c, x, z), index(to, tc, 1 - x, z)))
    return pairs


def near_route():
    return [(index(k, c, x, z), index(k, 1 - c, x, z)) for k, c, x, z in devices() if asks_near(c, x)]


def result_route(r):
    pairs = []
    for k, c, x, z in devices():
        v = (z + r * up_of(c)) % 4
        if (v > z) != bool(c):
            to, tc = k, 1 - c
        else:
            to, tc = partner_of(k, c)
        if 0 <= to < 8:
            pairs.append((index(k, c, x, z), index(to, tc, x, z)))
    return pairs


def send(value, route):
    return lax.ppermute(value, AXES, route)


def where_am_i():
    core = lax.rem(lax.axis_index("row"), 2)
    j = lax.axis_index("col")
    return core, j, lax.div(j, 4), lax.rem(j, 4)


def around(z, core, ups):
    return lax.rem(z + 4 + jnp.where(core == 0, ups, -ups), 4)


def place(t, r):
    core, j, x, z = where_am_i()
    return core, j, (1 - x if t else x) * 4 + around(z, core, r)


def slot_for(neighbours, counts, offset):
    own = lax.axis_index("row") * COLS + lax.axis_index("col")
    slot = jnp.int32(NNB)
    for s in range(NNB):
        hit = (neighbours[0, s] == own + offset) & (s < counts[0])
        slot = jnp.where(hit, s, slot)
    return slot


def result_slot(neighbours, counts, t, r, opposite):
    _, j, v = place(t, -r if opposite else r)
    return slot_for(neighbours, counts, jnp.where(v < j, 8 + v - j, v - j - 8))


def columns(c):
    return pl.ds(c * KS, KS)


def load(parts, target, sem):
    return [
        pltpu.make_async_copy(ref.at[i], target.at[:, columns(c)], sem)
        for c, (ref, i) in enumerate(parts)
    ]


MIRROR = (0, 3, 2, 1, 4, 7, 6, 5)


def load_mirrored(whole, target, sem, halves=0):
    return [
        pltpu.make_async_copy(whole.at[:, columns((m + halves) % COLS)], target.at[:, columns(c)], sem)
        for c, m in enumerate(MIRROR)
    ]


def multiply(left, right, result):
    def step(n, _):
        rows = pl.ds(pl.multiple_of(n * TILE, TILE), TILE)
        result[:, rows] = lax.dot_general(
            left[...], right[rows, :], (((1,), (1,)), ((), ())), preferred_element_type=jnp.float32
        ).astype(jnp.bfloat16)
        return 0

    lax.fori_loop(0, BS // TILE, step, 0)


def pick_kernel(block_order, coeffs, a0, y0, a1, y1, sem):
    core, _, x, z = where_am_i()
    base = lax.axis_index("row") * COLS
    copies = []
    for t, (a, y) in enumerate(((a0, y0), (a1, y1))):
        for ref, rs in ((a, (2, 1)), (y, (3, 0))):
            for i, r in enumerate(rs):
                v = (1 - x if t else x) * 4 + around(z, core, r)
                copies.append(pltpu.make_async_copy(coeffs.at[block_order[base + v] - base], ref.at[i], sem))
    for copy in copies:
        copy.start()
    for copy in copies:
        copy.wait()


def n_arrays(where):
    return max(i for parts in where for i, _ in parts) + 1


def weigh_kernel(where, occupations, *rest):
    refs, (out, block, sem) = rest[:-3], rest[-3:]
    copies = load([(refs[n], i) for n, i in where[0]], block, sem)
    for copy in copies:
        copy.start()
    for copy in copies:
        copy.wait()
    core, _, x, z = where_am_i()
    for c in range(COLS):
        ups = (0, -1, -2, 1)[c % 4]
        source = (1 - x if c // 4 else x) * 4 + around(z, core, ups)
        scale = occupations[pl.ds(source, 1), :]
        out[:, columns(c)] = (block[:, columns(c)].astype(jnp.float32) * scale).astype(jnp.bfloat16)


def own_kernel(blocks, first, where, neighbours, counts, weights, *rest):
    n = len(blocks)
    refs, rest = rest[: n_arrays(where)], rest[n_arrays(where) :]
    if not first:
        rest = rest[1:]
    out, left, right, result, left_sem, sem, out_sem = rest
    slots = []
    for b, (t, r) in enumerate(blocks):
        _, j, v = place(t, r)
        slots.append(slot_for(neighbours, counts, v - j))
    pltpu.make_async_copy(weights, left, left_sem).start()
    for b in range(n):
        @pl.when(slots[b] < NNB)
        def _():
            for copy in load([(refs[i], p) for i, p in where[b]], right.at[b], sem.at[b]):
                copy.start()

    if first:
        result[0] = jnp.zeros((BS, BS), jnp.bfloat16)
        for s in range(NNB):
            @pl.when(s >= counts[0])
            def _():
                pltpu.make_async_copy(result.at[0], out.at[s], out_sem.at[0]).start()
        for s in range(NNB):
            @pl.when(s >= counts[0])
            def _():
                pltpu.make_async_copy(result.at[0], out.at[s], out_sem.at[0]).wait()
    pltpu.make_async_copy(weights, left, left_sem).wait()
    for b in range(n):
        @pl.when(slots[b] < NNB)
        def _():
            for copy in load([(refs[i], p) for i, p in where[b]], right.at[b], sem.at[b]):
                copy.wait()
            multiply(left, right.at[b], result.at[b])
            pltpu.make_async_copy(result.at[b], out.at[slots[b]], out_sem.at[b]).start()
    for b in range(n):
        @pl.when(slots[b] < NNB)
        def _():
            pltpu.make_async_copy(result.at[b], out.at[slots[b]], out_sem.at[b]).wait()


def ask_kernel(blocks, where, lefts, *rest):
    n = len(blocks)
    left_refs, rest = rest[:lefts], rest[lefts:]
    refs, rest = rest[: n_arrays(where)], rest[n_arrays(where) :]
    outs, (left, right, left_sem, sem) = rest[:-4], rest[-4:]
    core, _, x, _ = where_am_i()
    plane = (lax.rem(lax.div(lax.axis_index("row"), 2), 2) == 0) != (core == 0)

    def body():
        left_copies = load_mirrored(left_refs[0], left.at[0], left_sem, 4 if lefts == 1 else 0)
        copies = [load([(refs[i], p) for i, p in where[b]], right.at[b], sem.at[b]) for b in range(n)]
        for copy in left_copies + [c for row in copies for c in row]:
            copy.start()
        if lefts > 1:
            for wanted, ref in ((plane, left_refs[1]), (jnp.logical_not(plane), left_refs[2])):
                @pl.when(wanted)
                def _():
                    for copy in load_mirrored(ref, left.at[1], left_sem):
                        copy.start()

            left_copies += load_mirrored(left_refs[1], left.at[1], left_sem)
        for copy in left_copies:
            copy.wait()
        for b in range(n):
            for copy in copies[b]:
                copy.wait()
            if lefts == 1:
                multiply(left.at[0], right.at[b], outs[0].at[b])
            else:
                _, j, v = place(*blocks[b])
                chosen = jnp.where(jnp.where(core == 0, v > j, v < j), 0, 1)
                multiply(left.at[chosen], right.at[b], outs[b])

    if lefts == 1:
        pl.when((core == 0) == (x == 0))(body)
    else:
        body()


def both_kernel(blocks, where, neighbours, counts, weights, near, *rest):
    n = len(blocks)
    refs, (_, out, answers, left, right, result, left_sem, sem, out_sem) = rest[:-9], rest[-9:]
    core, j, x, _ = where_am_i()
    asks = (core == 0) == (x == 0)
    slots = [slot_for(neighbours, counts, place(t, r)[2] - j) for t, r in blocks]
    copies = [load([(refs[i], p) for i, p in where[b]], right.at[b], sem.at[b]) for b in range(n)]

    @pl.when(asks)
    def _():
        for copy in load_mirrored(near, left.at[0], left_sem.at[0]):
            copy.start()

    for copy in [c for row in copies for c in row]:
        copy.start()
    pltpu.make_async_copy(weights, left.at[1], left_sem.at[1]).start()

    @pl.when(asks)
    def _():
        for copy in load_mirrored(near, left.at[0], left_sem.at[0]):
            copy.wait()

    for b in range(n):
        for copy in copies[b]:
            copy.wait()

        @pl.when(asks)
        def _():
            multiply(left.at[0], right.at[b], answers.at[b])

    pltpu.make_async_copy(weights, left.at[1], left_sem.at[1]).wait()
    for b in range(n):
        @pl.when(slots[b] < NNB)
        def _():
            multiply(left.at[1], right.at[b], result.at[b])
            pltpu.make_async_copy(result.at[b], out.at[slots[b]], out_sem.at[b]).start()
    for b in range(n):
        @pl.when(slots[b] < NNB)
        def _():
            pltpu.make_async_copy(result.at[b], out.at[slots[b]], out_sem.at[b]).wait()


def gather_kernel(steps, where, neighbours, counts, *rest):
    n = len(steps)
    refs, (_, out, held, sem, out_sem) = rest[:-5], rest[-5:]
    sources = [refs[i] if p is None else refs[i].at[p] for i, p in where]
    core, _, x, _ = where_am_i()
    from_across = (core == 0) == (x == 0)
    slots = []
    for i, (t, r, kind) in enumerate(steps):
        slot = result_slot(neighbours, counts, t, r, True)
        if kind:
            slot = jnp.where(from_across if kind == "across" else jnp.logical_not(from_across), slot, NNB)
        slots.append(slot)

        @pl.when(slot < NNB)
        def _():
            pltpu.make_async_copy(sources[i], held.at[i], sem.at[i]).start()

    for i in range(n):
        @pl.when(slots[i] < NNB)
        def _():
            pltpu.make_async_copy(sources[i], held.at[i], sem.at[i]).wait()
            pltpu.make_async_copy(held.at[i], out.at[slots[i]], out_sem.at[i]).start()

    for i in range(n):
        @pl.when(slots[i] < NNB)
        def _():
            pltpu.make_async_copy(held.at[i], out.at[slots[i]], out_sem.at[i]).wait()


ANY = pl.BlockSpec(memory_space=pl.ANY)
SMEM = pl.BlockSpec(memory_space=pltpu.SMEM)
VMEM = pl.BlockSpec(memory_space=pltpu.VMEM)
OUT = jax.ShapeDtypeStruct((NNB, BS, BS), jnp.bfloat16)
RESULT = jax.ShapeDtypeStruct((BS, BS), jnp.bfloat16)
PAIR = jax.ShapeDtypeStruct((2, BS, KS), jnp.bfloat16)
WHOLE = jax.ShapeDtypeStruct((BS, STATES), jnp.bfloat16)
BLOCK = pltpu.VMEM((BS, STATES), jnp.bfloat16)


def cost(n):
    return pl.CostEstimate(flops=n * 2 * BS * BS * STATES, bytes_accessed=n * 9 * BS * BS, transcendentals=0)


def limit(mib):
    return pltpu.CompilerParams(vmem_limit_bytes=mib << 20)


def pick(block_order, coeffs):
    return pl.pallas_call(
        pick_kernel,
        out_shape=[PAIR] * 4,
        in_specs=[SMEM, ANY],
        out_specs=[VMEM] * 4,
        scratch_shapes=[pltpu.SemaphoreType.DMA],
        compiler_params=limit(8),
        name="pick",
    )(block_order, coeffs)


def distinct(blocks):
    arrays, where = [], []
    for parts in blocks:
        row = []
        for array, position in parts:
            n = next((i for i, other in enumerate(arrays) if other is array), len(arrays))
            if n == len(arrays):
                arrays.append(array)
            row.append((n, position))
        where.append(tuple(row))
    return arrays, tuple(where)


def weigh(occupations, parts):
    arrays, where = distinct([parts])
    return pl.pallas_call(
        functools.partial(weigh_kernel, where),
        out_shape=WHOLE,
        in_specs=[VMEM] + [ANY] * len(arrays),
        out_specs=VMEM,
        scratch_shapes=[BLOCK, pltpu.SemaphoreType.DMA],
        compiler_params=limit(12),
        name="weigh",
    )(occupations, *arrays)


def own_products(blocks, neighbours, counts, weights, parts, out):
    first = out is None
    extra = [] if first else [out]
    arrays, where = distinct(parts)
    m, n = len(arrays), len(blocks)
    return pl.pallas_call(
        functools.partial(own_kernel, blocks, first, where),
        out_shape=OUT,
        in_specs=[SMEM, SMEM] + [ANY] * (1 + m + len(extra)),
        out_specs=ANY,
        scratch_shapes=[
            BLOCK, pltpu.VMEM((n, BS, STATES), jnp.bfloat16), pltpu.VMEM((n, BS, BS), jnp.bfloat16),
            pltpu.SemaphoreType.DMA, pltpu.SemaphoreType.DMA((n,)), pltpu.SemaphoreType.DMA((n,)),
        ],
        input_output_aliases={} if first else {3 + m: 0},
        cost_estimate=cost(n),
        compiler_params=limit(20),
        name="own_products",
    )(neighbours, counts, weights, *arrays, *extra)


def ask_products(blocks, lefts, parts):
    arrays, where = distinct(parts)
    m, n = len(lefts), len(blocks)
    return pl.pallas_call(
        functools.partial(ask_kernel, blocks, where, m),
        out_shape=jax.ShapeDtypeStruct((n, BS, BS), jnp.bfloat16) if m == 1 else [RESULT] * n,
        in_specs=[ANY] * (m + len(arrays)),
        out_specs=VMEM if m == 1 else [VMEM] * n,
        scratch_shapes=[
            pltpu.VMEM((min(m, 2), BS, STATES), jnp.bfloat16),
            pltpu.VMEM((n, BS, STATES), jnp.bfloat16),
            pltpu.SemaphoreType.DMA, pltpu.SemaphoreType.DMA((n,)),
        ],
        cost_estimate=cost(n),
        compiler_params=limit(20),
        name="ask_products",
    )(*lefts, *arrays)


def both_products(blocks, neighbours, counts, weights, near, parts, out):
    arrays, where = distinct(parts)
    m, n = len(arrays), len(blocks)
    return pl.pallas_call(
        functools.partial(both_kernel, blocks, where),
        out_shape=[OUT, jax.ShapeDtypeStruct((n, BS, BS), jnp.bfloat16)],
        in_specs=[SMEM, SMEM] + [ANY] * (3 + m),
        out_specs=[ANY, VMEM],
        scratch_shapes=[
            pltpu.VMEM((2, BS, STATES), jnp.bfloat16),
            pltpu.VMEM((n, BS, STATES), jnp.bfloat16),
            pltpu.VMEM((n, BS, BS), jnp.bfloat16),
            pltpu.SemaphoreType.DMA((2,)), pltpu.SemaphoreType.DMA((n,)), pltpu.SemaphoreType.DMA((n,)),
        ],
        input_output_aliases={4 + m: 0},
        cost_estimate=cost(2 * n),
        compiler_params=limit(20),
        name="both_products",
    )(neighbours, counts, weights, near, *arrays, out)


def gather(steps, neighbours, counts, results, out):
    arrays, where = distinct([results])
    n = len(steps)
    return pl.pallas_call(
        functools.partial(gather_kernel, steps, where[0]),
        out_shape=OUT,
        in_specs=[SMEM, SMEM] + [ANY] * (len(arrays) + 1),
        out_specs=ANY,
        scratch_shapes=[
            pltpu.VMEM((n, BS, BS), jnp.bfloat16),
            pltpu.SemaphoreType.DMA((n,)), pltpu.SemaphoreType.DMA((n,)),
        ],
        input_output_aliases={2 + len(arrays): 0},
        compiler_params=limit(10),
        name="place_results",
    )(neighbours, counts, *arrays, out)


def shards(coeffs, occupations, block_order, neighbours, counts):
    local = pick(block_order, coeffs.reshape(COLS, BS, KS))
    held = {("O", 0, "A"): local[0], ("O", 0, "Y"): local[1], ("O", 1, "A"): local[2], ("O", 1, "Y"): local[3]}
    up, down, far_up = {}, {}, {}
    for t in range(2):
        for part in "AY":
            held["P", t, part] = send(held["O", 1 - t, part], move_route(1, 0))
    for key in [(x, t, part) for t in range(2) for x in "OP" for part in "AY"]:
        up[key] = send(held[key], move_route(0, 1))
        down[key] = send(held[key], move_route(0, -1))
        if key == ("O", 1, "Y"):
            far_up[key] = send(far_up["P", 0, "Y"], move_route(1, 0))
        else:
            far_up[key] = send(up[key], move_route(0, 1))

    own_at = {2: ("A", 0), 1: ("A", 1), 3: ("Y", 0), 0: ("Y", 1)}

    def parts_of(t, r):
        parts = []
        for x in "OP":
            for table, shift in ((held, 0), (up, 1), (far_up, 2), (down, -1)):
                part, position = own_at[(r + shift) % 4]
                parts.append((table[x, t, part], position))
        return parts

    weights = weigh(occupations.reshape(COLS, KS), parts_of(0, 0))
    near = send(weights, swap_route())
    far_in = send(weights, edge_route())
    along_y, along_x = plane_routes()
    far_out = send(send(weights, along_y), along_x)
    across = send(weights, across_route())
    out = own_products(((0, 0),), neighbours, counts, weights, [parts_of(0, 0)], None)

    rest = ((0, 3), (0, 1), (0, 2))
    parts = [parts_of(*b) for b in rest]
    out = own_products(rest, neighbours, counts, weights, parts, out)
    answers = ask_products(rest, [near, far_in, far_out], parts)
    back = [(send(a, result_route(b[1])), None) for a, b in zip(answers, rest)]
    steps = [(0, r, None) for _, r in rest]
    whole = ((0, 3), (0, 0), (0, 1), (0, 2))
    answer = ask_products(whole, [across], [parts_of(*b) for b in whole])
    answer = send(answer, across_route())
    back += [(answer, i) for i in range(4)]
    steps += [(1, r, "across") for _, r in whole]
    for pair in (((1, 0), (1, 3)), ((1, 1), (1, 2))):
        parts = [parts_of(*b) for b in pair]
        out, answer = both_products(pair, neighbours, counts, weights, near, parts, out)
        answer = send(answer, near_route())
        back += [(answer, 0), (answer, 1)]
        steps += [(1, r, "near") for _, r in pair]
    out = gather(tuple(steps[:7]), neighbours, counts, back[:7], out)
    out = gather(tuple(steps[7:]), neighbours, counts, back[7:], out)
    return out[None]


def solution(mesh):
    return jax.shard_map(
        shards,
        mesh=mesh,
        in_specs=(P("row", "col"), P(), P(), P(("row", "col"), None), P(("row", "col"))),
        out_specs=P(("row", "col"), None, None, None),
        check_vma=False,
    )
```

```python
import functools

import jax
import jax.numpy as jnp
from jax import lax
from jax.experimental import pallas as pl
from jax.experimental.pallas import tpu as pltpu
from jax.sharding import PartitionSpec as P


NNB = 15
BS = 512
COLS = 8
KS = 256
STATES = COLS * KS
AXES = ("row", "col")
TILE = 256


def devices():
    for k in range(8):
        for core in range(2):
            for xh in range(2):
                for z in range(4):
                    yield k, core, xh, z


def index(k, core, xh, z):
    return ((k * 2 + core) * 2 + xh) * 4 + z


def up_of(core):
    return -1 if core else 1


def move_route(dx, up):
    return [
        (index(k, c, x ^ dx, (z - up * up_of(c)) % 4), index(k, c, x, z)) for k, c, x, z in devices()
    ]


def swap_route():
    return [(index(k, c, x, z), index(k, 1 - c, x, z)) for k, c, x, z in devices()]


def partner_of(k, core):
    return (k + 1, 0) if core else (k - 1, 1)


def in_plane(k, core):
    return (k % 2 == 0) != (core == 0)


def edge_route():
    pairs = []
    for k, c, x, z in devices():
        to, tc = partner_of(k, c)
        if 0 <= to < 8 and in_plane(k, c):
            pairs.append((index(k, c, x, z), index(to, tc, x, z)))
    return pairs


def plane_routes():
    first, second = [], []
    for k, c, x, z in devices():
        to, tc = partner_of(k, c)
        if 0 <= to < 8 and not in_plane(k, c):
            middle = index(2 * to - k, c, x, z)
            first.append((index(k, c, x, z), middle))
            second.append((middle, index(to, tc, x, z)))
    return first, second


def asks_near(core, xh):
    return (core == 0) == (xh == 0)


def across_route():
    pairs = []
    for k, c, x, z in devices():
        to, tc = partner_of(k, c)
        if 0 <= to < 8 and asks_near(c, x):
            pairs.append((index(k, c, x, z), index(to, tc, 1 - x, z)))
    return pairs


def answer_routes():
    direct, first, second = [], [], []
    for k, c, x, z in devices():
        to, tc = partner_of(k, c)
        if 0 <= to < 8 and asks_near(c, x):
            here, there = index(k, c, x, z), index(to, tc, 1 - x, z)
            if in_plane(k, c):
                direct.append((here, there))
            else:
                middle = index(2 * to - k, c, x, z)
                first.append((here, middle))
                second.append((middle, there))
    return direct, first, second


def near_route():
    return [(index(k, c, x, z), index(k, 1 - c, x, z)) for k, c, x, z in devices() if asks_near(c, x)]


def result_route(r):
    pairs = []
    for k, c, x, z in devices():
        v = (z + r * up_of(c)) % 4
        if (v > z) != bool(c):
            to, tc = k, 1 - c
        else:
            to, tc = partner_of(k, c)
        if 0 <= to < 8:
            pairs.append((index(k, c, x, z), index(to, tc, x, z)))
    return pairs


def send(value, route):
    return lax.ppermute(value, AXES, route)


def where_am_i():
    core = lax.rem(lax.axis_index("row"), 2)
    j = lax.axis_index("col")
    return core, j, lax.div(j, 4), lax.rem(j, 4)


def around(z, core, ups):
    return lax.rem(z + 4 + jnp.where(core == 0, ups, -ups), 4)


def place(t, r):
    core, j, x, z = where_am_i()
    return core, j, (1 - x if t else x) * 4 + around(z, core, r)


def slot_for(neighbours, counts, offset):
    own = lax.axis_index("row") * COLS + lax.axis_index("col")
    slot = jnp.int32(NNB)
    for s in range(NNB):
        hit = (neighbours[0, s] == own + offset) & (s < counts[0])
        slot = jnp.where(hit, s, slot)
    return slot


def result_slot(neighbours, counts, t, r, opposite):
    _, j, v = place(t, -r if opposite else r)
    return slot_for(neighbours, counts, jnp.where(v < j, 8 + v - j, v - j - 8))


def columns(c):
    return pl.ds(c * KS, KS)


def load(parts, target, sem):
    return [
        pltpu.make_async_copy(ref.at[i], target.at[:, columns(c)], sem)
        for c, (ref, i) in enumerate(parts)
    ]


MIRROR = (0, 3, 2, 1, 4, 7, 6, 5)


def load_mirrored(whole, target, sem, halves=0):
    return [
        pltpu.make_async_copy(whole.at[:, columns((m + halves) % COLS)], target.at[:, columns(c)], sem)
        for c, m in enumerate(MIRROR)
    ]


def multiply(left, right, result):
    def step(n, _):
        rows = pl.ds(pl.multiple_of(n * TILE, TILE), TILE)
        result[:, rows] = lax.dot_general(
            left[...], right[rows, :], (((1,), (1,)), ((), ())), preferred_element_type=jnp.float32
        ).astype(jnp.bfloat16)
        return 0

    lax.fori_loop(0, BS // TILE, step, 0)


def pick_kernel(block_order, coeffs, a0, y0, a1, y1, sem):
    core, _, x, z = where_am_i()
    base = lax.axis_index("row") * COLS
    copies = []
    for t, (a, y) in enumerate(((a0, y0), (a1, y1))):
        for ref, rs in ((a, (2, 1)), (y, (3, 0))):
            for i, r in enumerate(rs):
                v = (1 - x if t else x) * 4 + around(z, core, r)
                copies.append(pltpu.make_async_copy(coeffs.at[block_order[base + v] - base], ref.at[i], sem))
    for copy in copies:
        copy.start()
    for copy in copies:
        copy.wait()


def n_arrays(where):
    return max(i for parts in where for i, _ in parts) + 1


def weigh_kernel(where, occupations, *rest):
    refs, (out, block, sem) = rest[:-3], rest[-3:]
    copies = load([(refs[n], i) for n, i in where[0]], block, sem)
    for copy in copies:
        copy.start()
    for copy in copies:
        copy.wait()
    core, _, x, z = where_am_i()
    for c in range(COLS):
        ups = (0, -1, -2, 1)[c % 4]
        source = (1 - x if c // 4 else x) * 4 + around(z, core, ups)
        scale = occupations[pl.ds(source, 1), :]
        out[:, columns(c)] = (block[:, columns(c)].astype(jnp.float32) * scale).astype(jnp.bfloat16)


def own_kernel(blocks, first, where, neighbours, counts, weights, *rest):
    n = len(blocks)
    refs, rest = rest[: n_arrays(where)], rest[n_arrays(where) :]
    if not first:
        rest = rest[1:]
    out, left, right, result, left_sem, sem, out_sem = rest
    slots = []
    for b, (t, r) in enumerate(blocks):
        _, j, v = place(t, r)
        slots.append(slot_for(neighbours, counts, v - j))
    pltpu.make_async_copy(weights, left, left_sem).start()
    for b in range(n):
        @pl.when(slots[b] < NNB)
        def _():
            for copy in load([(refs[i], p) for i, p in where[b]], right.at[b], sem.at[b]):
                copy.start()

    if first:
        result[0] = jnp.zeros((BS, BS), jnp.bfloat16)
        for s in range(NNB):
            @pl.when(s >= counts[0])
            def _():
                pltpu.make_async_copy(result.at[0], out.at[s], out_sem.at[0]).start()
        for s in range(NNB):
            @pl.when(s >= counts[0])
            def _():
                pltpu.make_async_copy(result.at[0], out.at[s], out_sem.at[0]).wait()
    pltpu.make_async_copy(weights, left, left_sem).wait()
    for b in range(n):
        @pl.when(slots[b] < NNB)
        def _():
            for copy in load([(refs[i], p) for i, p in where[b]], right.at[b], sem.at[b]):
                copy.wait()
            multiply(left, right.at[b], result.at[b])
            pltpu.make_async_copy(result.at[b], out.at[slots[b]], out_sem.at[b]).start()
    for b in range(n):
        @pl.when(slots[b] < NNB)
        def _():
            pltpu.make_async_copy(result.at[b], out.at[slots[b]], out_sem.at[b]).wait()


def ask_kernel(blocks, where, lefts, *rest):
    n = len(blocks)
    left_refs, rest = rest[:lefts], rest[lefts:]
    refs, rest = rest[: n_arrays(where)], rest[n_arrays(where) :]
    outs, (left, right, left_sem, sem) = rest[:-4], rest[-4:]
    core, _, x, _ = where_am_i()
    plane = (lax.rem(lax.div(lax.axis_index("row"), 2), 2) == 0) != (core == 0)

    def body():
        left_copies = load_mirrored(left_refs[0], left.at[0], left_sem, 4 if lefts == 1 else 0)
        copies = [load([(refs[i], p) for i, p in where[b]], right.at[b], sem.at[b]) for b in range(n)]
        for copy in left_copies + [c for row in copies for c in row]:
            copy.start()
        if lefts > 1:
            for wanted, ref in ((plane, left_refs[1]), (jnp.logical_not(plane), left_refs[2])):
                @pl.when(wanted)
                def _():
                    for copy in load_mirrored(ref, left.at[1], left_sem):
                        copy.start()

            left_copies += load_mirrored(left_refs[1], left.at[1], left_sem)
        for copy in left_copies:
            copy.wait()
        for b in range(n):
            for copy in copies[b]:
                copy.wait()
            if lefts == 1:
                multiply(left.at[0], right.at[b], outs[0].at[b])
            else:
                _, j, v = place(*blocks[b])
                chosen = jnp.where(jnp.where(core == 0, v > j, v < j), 0, 1)
                multiply(left.at[chosen], right.at[b], outs[b])

    if lefts == 1:
        pl.when((core == 0) == (x == 0))(body)
    else:
        body()


def both_kernel(blocks, where, neighbours, counts, weights, near, *rest):
    n = len(blocks)
    refs, (_, out, answers, left, right, result, left_sem, sem, out_sem) = rest[:-9], rest[-9:]
    core, j, x, _ = where_am_i()
    asks = (core == 0) == (x == 0)
    slots = [slot_for(neighbours, counts, place(t, r)[2] - j) for t, r in blocks]
    copies = [load([(refs[i], p) for i, p in where[b]], right.at[b], sem.at[b]) for b in range(n)]

    @pl.when(asks)
    def _():
        for copy in load_mirrored(near, left.at[0], left_sem.at[0]):
            copy.start()

    for copy in [c for row in copies for c in row]:
        copy.start()
    pltpu.make_async_copy(weights, left.at[1], left_sem.at[1]).start()

    @pl.when(asks)
    def _():
        for copy in load_mirrored(near, left.at[0], left_sem.at[0]):
            copy.wait()

    for b in range(n):
        for copy in copies[b]:
            copy.wait()

        @pl.when(asks)
        def _():
            multiply(left.at[0], right.at[b], answers.at[b])

    pltpu.make_async_copy(weights, left.at[1], left_sem.at[1]).wait()
    for b in range(n):
        @pl.when(slots[b] < NNB)
        def _():
            multiply(left.at[1], right.at[b], result.at[b])
            pltpu.make_async_copy(result.at[b], out.at[slots[b]], out_sem.at[b]).start()
    for b in range(n):
        @pl.when(slots[b] < NNB)
        def _():
            pltpu.make_async_copy(result.at[b], out.at[slots[b]], out_sem.at[b]).wait()


def gather_kernel(steps, where, neighbours, counts, *rest):
    n = len(steps)
    refs, (_, out, held, sem, out_sem) = rest[:-5], rest[-5:]
    sources = [refs[i] if p is None else refs[i].at[p] for i, p in where]
    core, _, x, _ = where_am_i()
    from_across = (core == 0) == (x == 0)
    plane = (lax.rem(lax.div(lax.axis_index("row"), 2), 2) == 0) != (core == 0)
    when = {
        "near": jnp.logical_not(from_across),
        "across": from_across & plane,
        "planes": from_across & jnp.logical_not(plane),
    }
    slots = []
    for i, (t, r, kind) in enumerate(steps):
        slot = result_slot(neighbours, counts, t, r, True)
        if kind:
            slot = jnp.where(when[kind], slot, NNB)
        slots.append(slot)

        @pl.when(slot < NNB)
        def _():
            pltpu.make_async_copy(sources[i], held.at[i], sem.at[i]).start()

    for i in range(n):
        @pl.when(slots[i] < NNB)
        def _():
            pltpu.make_async_copy(sources[i], held.at[i], sem.at[i]).wait()
            pltpu.make_async_copy(held.at[i], out.at[slots[i]], out_sem.at[i]).start()

    for i in range(n):
        @pl.when(slots[i] < NNB)
        def _():
            pltpu.make_async_copy(held.at[i], out.at[slots[i]], out_sem.at[i]).wait()


ANY = pl.BlockSpec(memory_space=pl.ANY)
SMEM = pl.BlockSpec(memory_space=pltpu.SMEM)
VMEM = pl.BlockSpec(memory_space=pltpu.VMEM)
OUT = jax.ShapeDtypeStruct((NNB, BS, BS), jnp.bfloat16)
RESULT = jax.ShapeDtypeStruct((BS, BS), jnp.bfloat16)
PAIR = jax.ShapeDtypeStruct((2, BS, KS), jnp.bfloat16)
WHOLE = jax.ShapeDtypeStruct((BS, STATES), jnp.bfloat16)
BLOCK = pltpu.VMEM((BS, STATES), jnp.bfloat16)


def cost(n):
    return pl.CostEstimate(flops=n * 2 * BS * BS * STATES, bytes_accessed=n * 9 * BS * BS, transcendentals=0)


def limit(mib):
    return pltpu.CompilerParams(vmem_limit_bytes=mib << 20)


def pick(block_order, coeffs):
    return pl.pallas_call(
        pick_kernel,
        out_shape=[PAIR] * 4,
        in_specs=[SMEM, ANY],
        out_specs=[VMEM] * 4,
        scratch_shapes=[pltpu.SemaphoreType.DMA],
        compiler_params=limit(8),
        name="pick",
    )(block_order, coeffs)


def distinct(blocks):
    arrays, where = [], []
    for parts in blocks:
        row = []
        for array, position in parts:
            n = next((i for i, other in enumerate(arrays) if other is array), len(arrays))
            if n == len(arrays):
                arrays.append(array)
            row.append((n, position))
        where.append(tuple(row))
    return arrays, tuple(where)


def weigh(occupations, parts):
    arrays, where = distinct([parts])
    return pl.pallas_call(
        functools.partial(weigh_kernel, where),
        out_shape=WHOLE,
        in_specs=[VMEM] + [ANY] * len(arrays),
        out_specs=VMEM,
        scratch_shapes=[BLOCK, pltpu.SemaphoreType.DMA],
        compiler_params=limit(12),
        name="weigh",
    )(occupations, *arrays)


def own_products(blocks, neighbours, counts, weights, parts, out):
    first = out is None
    extra = [] if first else [out]
    arrays, where = distinct(parts)
    m, n = len(arrays), len(blocks)
    return pl.pallas_call(
        functools.partial(own_kernel, blocks, first, where),
        out_shape=OUT,
        in_specs=[SMEM, SMEM] + [ANY] * (1 + m + len(extra)),
        out_specs=ANY,
        scratch_shapes=[
            BLOCK, pltpu.VMEM((n, BS, STATES), jnp.bfloat16), pltpu.VMEM((n, BS, BS), jnp.bfloat16),
            pltpu.SemaphoreType.DMA, pltpu.SemaphoreType.DMA((n,)), pltpu.SemaphoreType.DMA((n,)),
        ],
        input_output_aliases={} if first else {3 + m: 0},
        cost_estimate=cost(n),
        compiler_params=limit(20),
        name="own_products",
    )(neighbours, counts, weights, *arrays, *extra)


def ask_products(blocks, lefts, parts):
    arrays, where = distinct(parts)
    m, n = len(lefts), len(blocks)
    return pl.pallas_call(
        functools.partial(ask_kernel, blocks, where, m),
        out_shape=jax.ShapeDtypeStruct((n, BS, BS), jnp.bfloat16) if m == 1 else [RESULT] * n,
        in_specs=[ANY] * (m + len(arrays)),
        out_specs=VMEM if m == 1 else [VMEM] * n,
        scratch_shapes=[
            pltpu.VMEM((min(m, 2), BS, STATES), jnp.bfloat16),
            pltpu.VMEM((n, BS, STATES), jnp.bfloat16),
            pltpu.SemaphoreType.DMA, pltpu.SemaphoreType.DMA((n,)),
        ],
        cost_estimate=cost(n),
        compiler_params=limit(20),
        name="ask_products",
    )(*lefts, *arrays)


def both_products(blocks, neighbours, counts, weights, near, parts, out):
    arrays, where = distinct(parts)
    m, n = len(arrays), len(blocks)
    return pl.pallas_call(
        functools.partial(both_kernel, blocks, where),
        out_shape=[OUT, jax.ShapeDtypeStruct((n, BS, BS), jnp.bfloat16)],
        in_specs=[SMEM, SMEM] + [ANY] * (3 + m),
        out_specs=[ANY, VMEM],
        scratch_shapes=[
            pltpu.VMEM((2, BS, STATES), jnp.bfloat16),
            pltpu.VMEM((n, BS, STATES), jnp.bfloat16),
            pltpu.VMEM((n, BS, BS), jnp.bfloat16),
            pltpu.SemaphoreType.DMA((2,)), pltpu.SemaphoreType.DMA((n,)), pltpu.SemaphoreType.DMA((n,)),
        ],
        input_output_aliases={4 + m: 0},
        cost_estimate=cost(2 * n),
        compiler_params=limit(20),
        name="both_products",
    )(neighbours, counts, weights, near, *arrays, out)


def gather(steps, neighbours, counts, results, out):
    arrays, where = distinct([results])
    n = len(steps)
    return pl.pallas_call(
        functools.partial(gather_kernel, steps, where[0]),
        out_shape=OUT,
        in_specs=[SMEM, SMEM] + [ANY] * (len(arrays) + 1),
        out_specs=ANY,
        scratch_shapes=[
            pltpu.VMEM((n, BS, BS), jnp.bfloat16),
            pltpu.SemaphoreType.DMA((n,)), pltpu.SemaphoreType.DMA((n,)),
        ],
        input_output_aliases={2 + len(arrays): 0},
        compiler_params=limit(10),
        name="place_results",
    )(neighbours, counts, *arrays, out)


def shards(coeffs, occupations, block_order, neighbours, counts):
    local = pick(block_order, coeffs.reshape(COLS, BS, KS))
    held = {("O", 0, "A"): local[0], ("O", 0, "Y"): local[1], ("O", 1, "A"): local[2], ("O", 1, "Y"): local[3]}
    up, down, far_up = {}, {}, {}
    for t in range(2):
        for part in "AY":
            held["P", t, part] = send(held["O", 1 - t, part], move_route(1, 0))
    for key in [(x, t, part) for t in range(2) for x in "OP" for part in "AY"]:
        up[key] = send(held[key], move_route(0, 1))
        down[key] = send(held[key], move_route(0, -1))
        if key == ("O", 1, "Y"):
            far_up[key] = send(far_up["P", 0, "Y"], move_route(1, 0))
        else:
            far_up[key] = send(up[key], move_route(0, 1))

    own_at = {2: ("A", 0), 1: ("A", 1), 3: ("Y", 0), 0: ("Y", 1)}

    def parts_of(t, r):
        parts = []
        for x in "OP":
            for table, shift in ((held, 0), (up, 1), (far_up, 2), (down, -1)):
                part, position = own_at[(r + shift) % 4]
                parts.append((table[x, t, part], position))
        return parts

    weights = weigh(occupations.reshape(COLS, KS), parts_of(0, 0))
    near = send(weights, swap_route())
    far_in = send(weights, edge_route())
    along_y, along_x = plane_routes()
    far_out = send(send(weights, along_y), along_x)
    across = send(weights, across_route())
    out = own_products(((0, 0),), neighbours, counts, weights, [parts_of(0, 0)], None)

    rest = ((0, 3), (0, 1), (0, 2))
    parts = [parts_of(*b) for b in rest]
    out = own_products(rest, neighbours, counts, weights, parts, out)
    answers = ask_products(rest, [near, far_in, far_out], parts)
    back = [(send(a, result_route(b[1])), None) for a, b in zip(answers, rest)]
    steps = [(0, r, None) for _, r in rest]
    whole = ((0, 3), (0, 0), (0, 1), (0, 2))
    answer = ask_products(whole, [across], [parts_of(*b) for b in whole])
    direct, along_y, along_x = answer_routes()
    first = send(answer, along_y)
    for kind, got in (("across", send(answer, direct)), ("planes", send(first, along_x))):
        back += [(got, i) for i in range(4)]
        steps += [(1, r, kind) for _, r in whole]
    for pair in (((1, 0), (1, 3)), ((1, 1), (1, 2))):
        parts = [parts_of(*b) for b in pair]
        out, answer = both_products(pair, neighbours, counts, weights, near, parts, out)
        answer = send(answer, near_route())
        back += [(answer, 0), (answer, 1)]
        steps += [(1, r, "near") for _, r in pair]
    out = gather(tuple(steps[:11]), neighbours, counts, back[:11], out)
    out = gather(tuple(steps[11:]), neighbours, counts, back[11:], out)
    return out[None]


def solution(mesh):
    return jax.shard_map(
        shards,
        mesh=mesh,
        in_specs=(P("row", "col"), P(), P(), P(("row", "col"), None), P(("row", "col"))),
        out_specs=P(("row", "col"), None, None, None),
        check_vma=False,
    )
```
